32 devices in a mesh: gx: 4 (over y, x), gy: 4 (over z), gz: 2 (over core).
Axes of the slice: x: 2, y: 2, z: 4, core: 2. Of those that a mesh axis runs over, the one named last changes fastest.
Arguments:
- gas_pos: float32 [3, 4, 4, 2, 2048], P(None, 'gx', 'gy', 'gz'), may hold values from 0 to 1
- gas_mass: float32 [4, 4, 2, 2048], P('gx', 'gy', 'gz'), may hold values from 0.2 to 5
- source_pos: float32 [3, 4, 4, 2, 2048], P(None, 'gx', 'gy', 'gz'), may hold values from 0 to 1
- source_radius: float32 [4, 4, 2, 2048], P('gx', 'gy', 'gz'), may hold values from 0.25 to 1
- source_yield: float32 [2, 4, 4, 2, 2048], P(None, 'gx', 'gy', 'gz'), may hold values from 1 to 30
- source_momentum: float32 [3, 4, 4, 2, 2048], P(None, 'gx', 'gy', 'gz'), may hold values from -180 to 180
- source_tiles: int32 [4, 4, 2, 16, 8], P('gx', 'gy', 'gz'), may hold values from 0 to 431, as said below
- source_count: int32 [4, 4, 2], P('gx', 'gy', 'gz'), may hold values from 1 to 2048, as said below
Outputs:
- gas_gain: float32 [5, 4, 4, 2, 2048], P(None, 'gx', 'gy', 'gz')
The draws below stay inside these ranges and needn't reach their ends.
Inputs may be any that keep to these rules, and one draw needn't show every extreme that they name: `source_tiles`: the 8 tiles of one block lie one in each of the 8 domains around one corner of the block's domain (that domain among them), in increasing order. Over all blocks of one domain, at most 8 distinct listed tiles lie in any one neighbouring slot. `source_count`: some domain holds 2048 live sources in every draw.
All inputs are finite; a program needn't handle non-finite values.
Results may differ from the reference program's by a relative error of at most 0.0003.
Values sent between devices are 32-bit elements; how exact they have to be, the bound alone decides.
A program may use at most 64 MiB of HBM per device.

```python
import math
import jax
import jax.numpy as jnp
from jax import lax

GAS = 2048
SRC_BLOCKS = 16
TILES_LISTED = 8
GAS_TILES = 16
SOURCES = 2048
DOM_X = 4
DOM_Y = 4
DOM_Z = 2


def feedback_layout(key):
    base = jax.random.fold_in(key, 2024)
    streams = jax.random.split(base, 6)
    domains = DOM_X * DOM_Y * DOM_Z
    capacity = GAS_TILES // 2
    dom_ids = jnp.arange(domains, dtype=jnp.int32)
    counts = jax.random.randint(streams[0], (domains,), 1, SOURCES + 1)
    chosen = jax.random.randint(streams[1], (), 0, domains)
    counts = jnp.where(dom_ids == chosen, SOURCES, counts).astype(jnp.int32)
    scores = jax.random.randint(streams[2], (domains, 27, GAS_TILES), 0, 262144)
    scores = scores * GAS_TILES + jnp.arange(GAS_TILES, dtype=jnp.int32)[None, None, :]
    candidates = lax.top_k(scores, capacity)[1].astype(jnp.int32)
    corners = jax.random.randint(streams[3], (domains, SRC_BLOCKS), 0, 8)
    forced = jax.random.randint(streams[4], (), 0, 8)
    block_ids = jnp.arange(SRC_BLOCKS, dtype=jnp.int32)
    pinned = (dom_ids[:, None] == chosen) & (block_ids[None, :] < capacity)
    corners = jnp.where(pinned, forced, corners).astype(jnp.int32)
    rotate = jax.random.randint(streams[5], (domains, 27), 0, capacity)
    octant = jnp.arange(8, dtype=jnp.int32)
    sign_x = 2 * (corners // 4) - 1
    sign_y = 2 * (corners // 2 % 2) - 1
    sign_z = 2 * (corners % 2) - 1
    slots = 9 * (sign_x[:, :, None] * (octant // 4)[None, None, :] + 1)
    slots = slots + 3 * (sign_y[:, :, None] * (octant // 2 % 2)[None, None, :] + 1)
    slots = slots + (sign_z[:, :, None] * (octant % 2)[None, None, :] + 1)
    slot_flat = slots.reshape(domains, SRC_BLOCKS * 8)
    turned = jnp.take_along_axis(rotate, slot_flat, axis=1).reshape(domains, SRC_BLOCKS, 8)
    member = (block_ids[None, :, None] + turned) % capacity
    where_flat = (slots * capacity + member).reshape(domains, SRC_BLOCKS * 8)
    tiles = jnp.take_along_axis(candidates.reshape(domains, 27 * capacity), where_flat, axis=1)
    listed = slots * GAS_TILES + tiles.reshape(domains, SRC_BLOCKS, 8)
    listed = jnp.sort(listed, axis=-1).astype(jnp.int32)
    return (listed.reshape(DOM_X, DOM_Y, DOM_Z, SRC_BLOCKS, 8), counts.reshape(DOM_X, DOM_Y, DOM_Z))


def draw_source_tiles(key, part):
    return feedback_layout(key)[0]


def draw_source_count(key, part):
    return feedback_layout(key)[1]


def level_of(own_key, shape, shards, least, high):
    factor_of, own = 1.0, jax.random.fold_in(own_key, 6)
    for axis_at, shards_of in shards:
        draws = jnp.exp(jax.random.uniform(jax.random.fold_in(own, axis_at), (shards_of,), jnp.float32, least / len(shards), high / len(shards)))
        factor_of = factor_of * jnp.repeat(draws, shape[axis_at] // shards_of).reshape([-1 if axis == axis_at else 1 for axis in range(len(shape))])
    return factor_of


def normal_values(rng, extent, scale, bound, cuts=(), kind=jnp.bfloat16):
    level = level_of(rng, extent, cuts, -0.22, 0.18) if cuts else 1.0
    drawn = jax.random.normal(rng, extent, jnp.float32) * scale * level
    return jnp.minimum(jnp.maximum(drawn, -bound), bound).astype(kind)


def setup_inputs(seed: int = 0) -> dict:
    key_of = jax.random.split(jax.random.key(seed), 9)
    gas_pos = jnp.clip(1.0 * jax.random.uniform(key_of[0], (3, DOM_X, DOM_Y, DOM_Z, GAS), jnp.float32) ** level_of(key_of[0], (3, DOM_X, DOM_Y, DOM_Z, GAS), ((1, 4), (2, 4), (3, 2)), -0.2, 0.2), 0.0, 1.0)
    gas_mass = jnp.clip(jnp.exp(math.log(5.0) - 3.218876 * jax.random.uniform(key_of[1], (DOM_X, DOM_Y, DOM_Z, GAS), jnp.float32) ** level_of(key_of[1], (DOM_X, DOM_Y, DOM_Z, GAS), ((0, 4), (1, 4), (2, 2)), -0.2, 0.2)), 0.2, 5.0)
    source_pos = jnp.clip(1.0 * jax.random.uniform(key_of[2], (3, DOM_X, DOM_Y, DOM_Z, SOURCES), jnp.float32) ** level_of(key_of[2], (3, DOM_X, DOM_Y, DOM_Z, SOURCES), ((1, 4), (2, 4), (3, 2)), -0.2, 0.2), 0.0, 1.0)
    source_radius = jnp.clip(jnp.exp(math.log(1.0) - 1.3862944 * jax.random.uniform(key_of[3], (DOM_X, DOM_Y, DOM_Z, SOURCES), jnp.float32) ** level_of(key_of[3], (DOM_X, DOM_Y, DOM_Z, SOURCES), ((0, 4), (1, 4), (2, 2)), -0.2, 0.2)), 0.25, 1.0)
    source_yield = jnp.clip(jnp.exp(math.log(30.0) - 3.4011974 * jax.random.uniform(key_of[4], (2, DOM_X, DOM_Y, DOM_Z, SOURCES), jnp.float32) ** level_of(key_of[4], (2, DOM_X, DOM_Y, DOM_Z, SOURCES), ((1, 4), (2, 4), (3, 2)), -0.2, 0.2)), 1.0, 30.0)
    source_momentum = normal_values(key_of[5], (3, DOM_X, DOM_Y, DOM_Z, SOURCES), 30.0, 180.0, ((1, 4), (2, 4), (3, 2)), jnp.float32)
    source_tiles = draw_source_tiles(jax.random.fold_in(key_of[8], 71), 0)
    source_count = draw_source_count(jax.random.fold_in(key_of[8], 71), 0)
    return dict(gas_pos=gas_pos, gas_mass=gas_mass, source_pos=source_pos, source_radius=source_radius, source_yield=source_yield, source_momentum=source_momentum, source_tiles=source_tiles, source_count=source_count)


def block_deposit(near, tile_ids, source_xyz, inv_square, load, live, tiles_each):
    picked = jnp.take(near, tile_ids, axis=1)
    slot = tile_ids // tiles_each
    shifts = jnp.stack([slot // 9 - 1, (slot // 3) % 3 - 1, slot % 3 - 1]).astype(near.dtype)
    gas_xyz = (picked[0:3] + shifts[:, :, None]).reshape(3, -1)
    masses = picked[3].reshape(-1)
    dist_sq = jnp.square(gas_xyz[0][None, :] - source_xyz[0][:, None])
    dist_sq = dist_sq + jnp.square(gas_xyz[1][None, :] - source_xyz[1][:, None])
    dist_sq = dist_sq + jnp.square(gas_xyz[2][None, :] - source_xyz[2][:, None])
    weight = masses[None, :] / jnp.square(1.0 + dist_sq * inv_square[:, None])
    norm_sum = jnp.sum(weight, axis=1)
    coeffs = load * (live / norm_sum)[None, :]
    moved = jnp.dot(coeffs, weight, precision=lax.Precision.HIGHEST, preferred_element_type=jnp.float32)
    return moved.reshape(load.shape[0], tile_ids.shape[0], 128)


def reference(gas_pos, gas_mass, source_pos, source_radius, source_yield, source_momentum, source_tiles, source_count):
    gas_all = jnp.concatenate([gas_pos, gas_mass[None]], axis=0)
    load_all = jnp.concatenate([source_yield[0:1], source_momentum, source_yield[1:2]], axis=0)
    inv_all = (1.0 / jnp.square(source_radius))[None]
    zero = jnp.zeros((), jnp.int32)
    gain_init = jnp.zeros((5, DOM_X, DOM_Y, DOM_Z, GAS), jnp.float32)

    def per_device(gain, flat):
        ix = (flat // (DOM_Y * DOM_Z)).astype(jnp.int32)
        iy = ((flat // DOM_Z) % DOM_Y).astype(jnp.int32)
        iz = (flat % DOM_Z).astype(jnp.int32)
        starts = []
        for slot in range(27):
            sx = ((ix + slot // 9 - 1) % DOM_X).astype(jnp.int32)
            sy = ((iy + (slot // 3) % 3 - 1) % DOM_Y).astype(jnp.int32)
            sz = ((iz + slot % 3 - 1) % DOM_Z).astype(jnp.int32)
            starts.append((zero, sx, sy, sz, zero))
        pieces = [lax.dynamic_slice(gas_all, start, (4, 1, 1, 1, GAS)).reshape(4, GAS) for start in starts]
        near = jnp.stack(pieces, axis=1).reshape(4, 27 * GAS_TILES, 128)

        def own_rows(array):
            rows = lax.dynamic_slice(array, (zero, ix, iy, iz, zero), (array.shape[0], 1, 1, 1, SOURCES))
            return rows.reshape(array.shape[0], SRC_BLOCKS, 128)

        source_xyz = own_rows(source_pos)
        loads = own_rows(load_all)
        inv_sq = own_rows(inv_all)[0]
        tile_table = lax.dynamic_slice(source_tiles, (ix, iy, iz, zero, zero), (1, 1, 1, SRC_BLOCKS, TILES_LISTED)).reshape(SRC_BLOCKS, TILES_LISTED)
        live_count = lax.dynamic_slice(source_count, (ix, iy, iz), (1, 1, 1)).reshape(())
        used_blocks = ((live_count + 127) // 128).astype(jnp.int32)

        def add_block(block_idx, acc):
            live = (block_idx * 128 + jnp.arange(128, dtype=jnp.int32) < live_count).astype(gas_all.dtype)
            ids = lax.dynamic_index_in_dim(tile_table, block_idx, 0, keepdims=False)
            xyz_rows = lax.dynamic_index_in_dim(source_xyz, block_idx, 1, keepdims=False)
            inv_rows = lax.dynamic_index_in_dim(inv_sq, block_idx, 0, keepdims=False)
            load_rows = lax.dynamic_index_in_dim(loads, block_idx, 1, keepdims=False)
            moved = block_deposit(near, ids, xyz_rows, inv_rows, load_rows, live, GAS_TILES)
            return acc.at[:, ids].add(moved)

        acc_init = jnp.zeros((5, 27 * GAS_TILES, 128), jnp.float32)
        acc = lax.fori_loop(zero, used_blocks, add_block, acc_init)
        spread = acc.reshape(5, 27, GAS)
        for slot in range(27):
            current = lax.dynamic_slice(gain, starts[slot], (5, 1, 1, 1, GAS))
            gain = lax.dynamic_update_slice(gain, current + spread[:, slot].reshape(5, 1, 1, 1, GAS), starts[slot])
        return gain, None

    gain, unused_all = lax.scan(per_device, gain_init, jnp.arange(DOM_X * DOM_Y * DOM_Z, dtype=jnp.int32))
    return gain / gas_mass[None]
```

```python
import functools

import jax
import jax.numpy as jnp
from jax import lax
from jax.experimental import pallas as pl
from jax.experimental.pallas import tpu as pltpu
from jax.sharding import PartitionSpec as P


def kinds(count):
    return min(count, 3)


def kind_of(offset, count):
    if count >= 3:
        return offset + 1
    if count == 2:
        return jnp.abs(offset)
    return offset * 0


def up_pairs(count):
    return [(i, (i + 1) % count) for i in range(count)]


def down_pairs(count):
    return [((i + 1) % count, i) for i in range(count)]


def spread_axis(arr, axis, dim):
    count = lax.axis_size(axis)
    if count == 1:
        return arr
    if count == 2:
        return jnp.concatenate([arr, lax.ppermute(arr, axis, up_pairs(2))], axis=dim)
    before = lax.ppermute(arr, axis, up_pairs(count))
    after = lax.ppermute(arr, axis, down_pairs(count))
    return jnp.concatenate([before, arr, after], axis=dim)


def gather_axis(arr, axis, dim):
    count = lax.axis_size(axis)

    def at(i):
        return lax.index_in_dim(arr, i, axis=dim, keepdims=False)

    if count == 1:
        return at(0)
    if count == 2:
        return at(0) + lax.ppermute(at(1), axis, up_pairs(2))
    from_up = lax.ppermute(at(2), axis, up_pairs(count))
    from_down = lax.ppermute(at(0), axis, down_pairs(count))
    return at(1) + from_up + from_down


def split3(value):
    first = value.astype(jnp.bfloat16).astype(jnp.float32)
    rest = value - first
    second = rest.astype(jnp.bfloat16).astype(jnp.float32)
    return first, second, rest - second


def rows_of(rows):
    at = lax.broadcasted_iota(jnp.int32, (8, 128), 0)
    out = jnp.zeros((8, 128), jnp.float32)
    for i, row in enumerate(rows):
        out = jnp.where(at == i, row, out)
    return out


def deposit_kernel(sizes, tiles_each, unroll, table, count, near, pos, radius, yields, momentum, out, acc):
    blocks, listed = pos.shape[1], table.shape[1]
    slots = near.shape[0]
    nx, ny, nz = sizes
    acc[...] = jnp.zeros_like(acc)
    live_count = count[0]
    lane = lax.broadcasted_iota(jnp.int32, (1, 128), 1)

    def one_block(b):
        row = pl.ds(b, 1)
        r = radius[row, :]
        inv = 1.0 / (r * r)
        sx, sy, sz = (pos[k, row, :] - 0.5 for k in range(3))
        left = rows_of(
            [-2.0 * inv * sx, -2.0 * inv * sy, -2.0 * inv * sz, inv, 1.0 + inv * (sx * sx + sy * sy + sz * sz)]
        )
        a1, a2, a3 = split3(left)
        lhs = jnp.concatenate([a1, a1, a2, a2, a1, a3], axis=0).T.astype(jnp.bfloat16)
        norm_acc = jnp.zeros((128, 128), jnp.float32)
        high, low, places = [], [], []
        for j in range(listed):
            tile_id = table[b, j]
            slot, tile = tile_id // tiles_each, tile_id % tiles_each
            a, bb, c = slot // 9 - 1, slot // 3 % 3 - 1, slot % 3 - 1
            place = (kind_of(a, nx) * kinds(ny) + kind_of(bb, ny)) * kinds(nz) + kind_of(c, nz)
            places.append(place * tiles_each + tile)
            at = pl.ds(tile, 1)
            gx = near[place, 0, at, :] + (a.astype(jnp.float32) - 0.5)
            gy = near[place, 1, at, :] + (bb.astype(jnp.float32) - 0.5)
            gz = near[place, 2, at, :] + (c.astype(jnp.float32) - 0.5)
            mass = near[place, 3, at, :]
            b1, b2, b3 = split3(rows_of([gx, gy, gz, gx * gx + gy * gy + gz * gz, jnp.ones_like(gx)]))
            rhs = jnp.concatenate([b1, b2, b1, b2, b3, b1], axis=0).astype(jnp.bfloat16)
            u = jnp.dot(lhs, rhs, preferred_element_type=jnp.float32)
            w = 1.0 / (u * u)
            norm_acc = norm_acc + w * mass
            w1 = w.astype(jnp.bfloat16)
            high.append(w1)
            low.append((w - w1.astype(jnp.float32)).astype(jnp.bfloat16))
        norm = jnp.sum(norm_acc.T, axis=0, keepdims=True)
        live = jnp.where(b * 128 + lane < live_count, 1.0, 0.0)
        scale = live / norm
        loads = rows_of(
            [yields[0, row, :], momentum[0, row, :], momentum[1, row, :], momentum[2, row, :], yields[1, row, :]]
        )
        c1, c2, c3 = split3(loads * scale)
        coef = jnp.concatenate([c1, c2, c3, jnp.zeros_like(c1)], axis=0).astype(jnp.bfloat16)
        for j in range(listed):
            hi = jnp.dot(coef, high[j], preferred_element_type=jnp.float32)
            lo = jnp.dot(coef[0:16], low[j], preferred_element_type=jnp.float32)
            moved = hi[0:8] + (hi[8:16] + (hi[16:24] + (lo[0:8] + lo[8:16])))
            start = pl.multiple_of(places[j] * 8, 8)
            acc[pl.ds(start, 8), :] = acc[pl.ds(start, 8), :] + moved

    def step(i, carry):
        for k in range(unroll):
            one_block(i * unroll + k)
        return carry

    used = jnp.minimum((live_count + 127) // 128, blocks)
    lax.fori_loop(0, (used + unroll - 1) // unroll, step, 0)
    for slot in range(slots):
        for q in range(5):
            out[slot, q] = acc[pl.ds(slot * tiles_each * 8 + q, tiles_each, stride=8), :]


def local(sizes, gas_pos, gas_mass, source_pos, source_radius, source_yield, source_momentum, source_tiles, source_count):
    gas_size = gas_pos.shape[-1]
    tiles = gas_size // 128
    blocks = source_pos.shape[-1] // 128
    listed = source_tiles.shape[-1]
    nx, ny, nz = sizes
    slots = kinds(nx) * kinds(ny) * kinds(nz)
    gas = jnp.concatenate([gas_pos.reshape(3, tiles, 128), gas_mass.reshape(1, tiles, 128)], axis=0)
    near = gas.reshape(1, 1, 1, 4, tiles, 128)
    near = spread_axis(near, "gy", 1)
    near = spread_axis(near, "gx", 0)
    near = spread_axis(near, "gz", 2)
    near = near.reshape(slots, 4, tiles, 128)
    unroll = 2 if blocks % 2 == 0 else 1
    smem = pl.BlockSpec(memory_space=pltpu.SMEM)
    vmem = pl.BlockSpec(memory_space=pltpu.VMEM)
    moved = pl.pallas_call(
        functools.partial(deposit_kernel, sizes, tiles, unroll),
        out_shape=jax.ShapeDtypeStruct((slots, 5, tiles, 128), jnp.float32),
        in_specs=[smem, smem] + [vmem] * 5,
        out_specs=vmem,
        scratch_shapes=[pltpu.VMEM((slots * tiles * 8, 128), jnp.float32)],
    )(
        source_tiles.reshape(blocks, listed),
        source_count.reshape(1),
        near,
        source_pos.reshape(3, blocks, 128),
        source_radius.reshape(blocks, 128),
        source_yield.reshape(2, blocks, 128),
        source_momentum.reshape(3, blocks, 128),
    )
    moved = moved.reshape(kinds(nx), kinds(ny), kinds(nz), 5, tiles, 128)
    moved = gather_axis(moved, "gz", 2)
    moved = gather_axis(moved, "gx", 0)
    moved = gather_axis(moved, "gy", 0)
    return moved.reshape(5, 1, 1, 1, gas_size)


def solution(mesh):
    sizes = (mesh.shape["gx"], mesh.shape["gy"], mesh.shape["gz"])
    in_specs = (
        P(None, "gx", "gy", "gz", None),
        P("gx", "gy", "gz", None),
        P(None, "gx", "gy", "gz", None),
        P("gx", "gy", "gz", None),
        P(None, "gx", "gy", "gz", None),
        P(None, "gx", "gy", "gz", None),
        P("gx", "gy", "gz", None, None),
        P("gx", "gy", "gz"),
    )
    out_specs = P(None, "gx", "gy", "gz", None)
    return jax.shard_map(
        functools.partial(local, sizes), mesh=mesh, in_specs=in_specs, out_specs=out_specs, check_vma=False
    )
```

```python
import functools

import jax
import jax.numpy as jnp
from jax import lax
from jax.experimental import pallas as pl
from jax.experimental.pallas import tpu as pltpu
from jax.sharding import PartitionSpec as P


def kinds(count):
    return min(count, 3)


def kind_of(offset, count):
    if count >= 3:
        return offset + 1
    if count == 2:
        return jnp.abs(offset)
    return offset * 0


def own_kind(count):
    return 1 if count >= 3 else 0


def steps_of(count):
    if count >= 3:
        return ((0, -1), (2, 1))
    return ((1, 1),) if count == 2 else ()


AXES = ("gx", "gy", "gz")
MESH = pl.DeviceIdType.MESH


def neighbour(axis, count, step):
    return {axis: lax.rem(lax.axis_index(axis) + step + count, count)}


def greet(sizes):
    barrier = pltpu.get_barrier_semaphore()
    total = 0
    for axis, count in zip(AXES, sizes):
        for kind, step in steps_of(count):
            pl.semaphore_signal(barrier, inc=1, device_id=neighbour(axis, count, step), device_id_type=MESH)
            total += 1
    if total:
        pl.semaphore_wait(barrier, total)


def facing(kind, count):
    return 2 - kind if count >= 3 else kind


def spread_kernel(sizes, pos, mass, near, local_sem, send_sem, recv_sem):
    nx, ny, nz = sizes
    own = tuple(own_kind(n) for n in sizes)

    def place(i, j, k):
        return (i * kinds(ny) + j) * kinds(nz) + k

    home = place(*own)
    first = pltpu.make_async_copy(pos, near.at[home, pl.ds(0, 3)], local_sem.at[0])
    second = pltpu.make_async_copy(mass, near.at[home, pl.ds(3, 1)], local_sem.at[1])
    first.start()
    second.start()
    greet(sizes)
    first.wait()
    second.wait()
    copies = {}

    def pass_on(slot, dim):
        count = sizes[dim]
        for kind, step in steps_of(count):
            there = list(slot)
            there[dim] = facing(kind, count)
            target = place(*there)
            copy = pltpu.make_async_remote_copy(
                src_ref=near.at[place(*slot)],
                dst_ref=near.at[target],
                send_sem=send_sem.at[target],
                recv_sem=recv_sem.at[target],
                device_id=neighbour(AXES[dim], count, step),
                device_id_type=MESH,
            )
            copy.start()
            copies[tuple(there)] = copy

    order_y = [j for j in range(kinds(ny)) if j != own[1]]
    order_x = [i for i in range(kinds(nx)) if i != own[0]]
    order_z = [k for k in range(kinds(nz)) if k != own[2]]
    pass_on(own, 1)
    pass_on(own, 0)
    pass_on(own, 2)
    for j in order_y:
        slot = (own[0], j, own[2])
        copies[slot].wait_recv()
        pass_on(slot, 0)
        pass_on(slot, 2)
    for j in [own[1]] + order_y:
        for i in order_x:
            slot = (i, j, own[2])
            copies[slot].wait_recv()
            pass_on(slot, 2)
    for j in [own[1]] + order_y:
        for i in [own[0]] + order_x:
            for k in order_z:
                copies[(i, j, k)].wait_recv()
    for copy in copies.values():
        copy.wait_send()


def gather_kernel(sizes, moved, out, part, got_z, got_x, got_y, send_z, recv_z, send_x, recv_x, send_y, recv_y):
    nx, ny, nz = sizes
    own = tuple(own_kind(n) for n in sizes)

    def place(i, j, k):
        return (i * kinds(ny) + j) * kinds(nz) + k

    order_y = [j for j in range(kinds(ny)) if j != own[1]]
    order_x = [i for i in range(kinds(nx)) if i != own[0]]
    order_z = [k for k in range(kinds(nz)) if k != own[2]]
    columns = [(i, j) for j in order_y + [own[1]] for i in order_x]
    columns += [(own[0], j) for j in order_y + [own[1]]]
    greet(sizes)
    copies = []

    def send(src, dst, sends, recvs, at, dim, kind):
        count = sizes[dim]
        step = dict(steps_of(count))[kind]
        copy = pltpu.make_async_remote_copy(
            src_ref=src,
            dst_ref=dst,
            send_sem=sends.at[at],
            recv_sem=recvs.at[at],
            device_id=neighbour(AXES[dim], count, step),
            device_id_type=MESH,
        )
        copy.start()
        copies.append(copy)
        return copy

    along_z, along_x, along_y = {}, {}, {}
    for i, j in columns:
        for k in order_z:
            at = place(i, j, k)
            along_z[i, j, k] = send(moved.at[at], got_z.at[at], send_z, recv_z, at, 2, k)
    for i, j in columns:
        total = moved[place(i, j, own[2])]
        for k in order_z:
            along_z[i, j, k].wait_recv()
            total = total + got_z[place(i, j, k)]
        at = i * kinds(ny) + j
        part[at] = total
        if i != own[0]:
            along_x[i, j] = send(part.at[at], got_x.at[at], send_x, recv_x, at, 0, i)
    for j in order_y + [own[1]]:
        at = own[0] * kinds(ny) + j
        total = part[at]
        for i in order_x:
            along_x[i, j].wait_recv()
            total = total + got_x[i * kinds(ny) + j]
        part[at] = total
        if j != own[1]:
            along_y[j] = send(part.at[at], got_y.at[j], send_y, recv_y, j, 1, j)
    total = part[own[0] * kinds(ny) + own[1]]
    for j in order_y:
        along_y[j].wait_recv()
        total = total + got_y[j]
    out[...] = total
    for copy in copies:
        copy.wait_send()


def split3(value):
    first = value.astype(jnp.bfloat16).astype(jnp.float32)
    rest = value - first
    second = rest.astype(jnp.bfloat16).astype(jnp.float32)
    return first, second, rest - second


def rows_of(rows):
    at = lax.broadcasted_iota(jnp.int32, (8, 128), 0)
    out = jnp.zeros((8, 128), jnp.float32)
    for i, row in enumerate(rows):
        out = jnp.where(at == i, row, out)
    return out


def deposit_kernel(sizes, tiles_each, unroll, table, count, near, pos, radius, yields, momentum, out, acc):
    blocks, listed = pos.shape[1], table.shape[1]
    slots = near.shape[0]
    nx, ny, nz = sizes
    acc[...] = jnp.zeros_like(acc)
    live_count = count[0]
    lane = lax.broadcasted_iota(jnp.int32, (1, 128), 1)

    def one_block(b):
        row = pl.ds(b, 1)
        r = radius[row, :]
        inv = 1.0 / (r * r)
        sx, sy, sz = (pos[k, row, :] - 0.5 for k in range(3))
        left = rows_of(
            [-2.0 * inv * sx, -2.0 * inv * sy, -2.0 * inv * sz, inv, 1.0 + inv * (sx * sx + sy * sy + sz * sz)]
        )
        a1, a2, a3 = split3(left)
        lhs = jnp.concatenate([a1, a1, a2, a2, a1, a3], axis=0).T.astype(jnp.bfloat16)
        norm_acc = jnp.zeros((128, 128), jnp.float32)
        high, low, places = [], [], []
        for j in range(listed):
            tile_id = table[b, j]
            slot, tile = tile_id // tiles_each, tile_id % tiles_each
            a, bb, c = slot // 9 - 1, slot // 3 % 3 - 1, slot % 3 - 1
            place = (kind_of(a, nx) * kinds(ny) + kind_of(bb, ny)) * kinds(nz) + kind_of(c, nz)
            places.append(place * tiles_each + tile)
            at = pl.ds(tile, 1)
            gx = near[place, 0, at, :] + (a.astype(jnp.float32) - 0.5)
            gy = near[place, 1, at, :] + (bb.astype(jnp.float32) - 0.5)
            gz = near[place, 2, at, :] + (c.astype(jnp.float32) - 0.5)
            mass = near[place, 3, at, :]
            b1, b2, b3 = split3(rows_of([gx, gy, gz, gx * gx + gy * gy + gz * gz, jnp.ones_like(gx)]))
            rhs = jnp.concatenate([b1, b2, b1, b2, b3, b1], axis=0).astype(jnp.bfloat16)
            u = jnp.dot(lhs, rhs, preferred_element_type=jnp.float32)
            w = 1.0 / (u * u)
            norm_acc = norm_acc + w * mass
            w1 = w.astype(jnp.bfloat16)
            high.append(w1)
            low.append((w - w1.astype(jnp.float32)).astype(jnp.bfloat16))
        norm = jnp.sum(norm_acc.T, axis=0, keepdims=True)
        live = jnp.where(b * 128 + lane < live_count, 1.0, 0.0)
        scale = live / norm
        loads = rows_of(
            [yields[0, row, :], momentum[0, row, :], momentum[1, row, :], momentum[2, row, :], yields[1, row, :]]
        )
        c1, c2, c3 = split3(loads * scale)
        coef = jnp.concatenate([c1, c2, c3, jnp.zeros_like(c1)], axis=0).astype(jnp.bfloat16)
        for j in range(listed):
            hi = jnp.dot(coef, high[j], preferred_element_type=jnp.float32)
            lo = jnp.dot(coef[0:16], low[j], preferred_element_type=jnp.float32)
            moved = hi[0:8] + (hi[8:16] + (hi[16:24] + (lo[0:8] + lo[8:16])))
            start = pl.multiple_of(places[j] * 8, 8)
            acc[pl.ds(start, 8), :] = acc[pl.ds(start, 8), :] + moved

    def step(i, carry):
        for k in range(unroll):
            one_block(i * unroll + k)
        return carry

    used = jnp.minimum((live_count + 127) // 128, blocks)
    lax.fori_loop(0, (used + unroll - 1) // unroll, step, 0)
    for slot in range(slots):
        for q in range(5):
            out[slot, q] = acc[pl.ds(slot * tiles_each * 8 + q, tiles_each, stride=8), :]


def local(sizes, gas_pos, gas_mass, source_pos, source_radius, source_yield, source_momentum, source_tiles, source_count):
    gas_size = gas_pos.shape[-1]
    tiles = gas_size // 128
    blocks = source_pos.shape[-1] // 128
    listed = source_tiles.shape[-1]
    nx, ny, nz = sizes
    slots = kinds(nx) * kinds(ny) * kinds(nz)
    vmem = pl.BlockSpec(memory_space=pltpu.VMEM)
    near = pl.pallas_call(
        functools.partial(spread_kernel, sizes),
        out_shape=jax.ShapeDtypeStruct((slots, 4, tiles, 128), jnp.float32),
        in_specs=[vmem, vmem],
        out_specs=vmem,
        scratch_shapes=[
            pltpu.SemaphoreType.DMA((2,)),
            pltpu.SemaphoreType.DMA((slots,)),
            pltpu.SemaphoreType.DMA((slots,)),
        ],
        compiler_params=pltpu.CompilerParams(collective_id=0, has_side_effects=True),
    )(gas_pos.reshape(3, tiles, 128), gas_mass.reshape(1, tiles, 128))
    unroll = 2 if blocks % 2 == 0 else 1
    smem = pl.BlockSpec(memory_space=pltpu.SMEM)
    moved = pl.pallas_call(
        functools.partial(deposit_kernel, sizes, tiles, unroll),
        out_shape=jax.ShapeDtypeStruct((slots, 5, tiles, 128), jnp.float32),
        in_specs=[smem, smem] + [vmem] * 5,
        out_specs=vmem,
        scratch_shapes=[pltpu.VMEM((slots * tiles * 8, 128), jnp.float32)],
    )(
        source_tiles.reshape(blocks, listed),
        source_count.reshape(1),
        near,
        source_pos.reshape(3, blocks, 128),
        source_radius.reshape(blocks, 128),
        source_yield.reshape(2, blocks, 128),
        source_momentum.reshape(3, blocks, 128),
    )
    piece = (5, tiles, 128)
    sides = kinds(nx) * kinds(ny)
    gain = pl.pallas_call(
        functools.partial(gather_kernel, sizes),
        out_shape=jax.ShapeDtypeStruct(piece, jnp.float32),
        in_specs=[vmem],
        out_specs=vmem,
        scratch_shapes=[
            pltpu.VMEM((sides, *piece), jnp.float32),
            pltpu.VMEM((slots, *piece), jnp.float32),
            pltpu.VMEM((sides, *piece), jnp.float32),
            pltpu.VMEM((kinds(ny), *piece), jnp.float32),
            pltpu.SemaphoreType.DMA((slots,)),
            pltpu.SemaphoreType.DMA((slots,)),
            pltpu.SemaphoreType.DMA((sides,)),
            pltpu.SemaphoreType.DMA((sides,)),
            pltpu.SemaphoreType.DMA((kinds(ny),)),
            pltpu.SemaphoreType.DMA((kinds(ny),)),
        ],
        compiler_params=pltpu.CompilerParams(collective_id=1, has_side_effects=True),
    )(moved)
    return gain.reshape(5, 1, 1, 1, gas_size)


def solution(mesh):
    sizes = (mesh.shape["gx"], mesh.shape["gy"], mesh.shape["gz"])
    in_specs = (
        P(None, "gx", "gy", "gz", None),
        P("gx", "gy", "gz", None),
        P(None, "gx", "gy", "gz", None),
        P("gx", "gy", "gz", None),
        P(None, "gx", "gy", "gz", None),
        P(None, "gx", "gy", "gz", None),
        P("gx", "gy", "gz", None, None),
        P("gx", "gy", "gz"),
    )
    out_specs = P(None, "gx", "gy", "gz", None)
    return jax.shard_map(
        functools.partial(local, sizes), mesh=mesh, in_specs=in_specs, out_specs=out_specs, check_vma=False
    )
```

```python
import functools
import math

import jax
import jax.numpy as jnp
from jax import lax
from jax.experimental import pallas as pl
from jax.experimental.pallas import tpu as pltpu
from jax.sharding import PartitionSpec as P


def kinds(count):
    return min(count, 3)


def kind_of(offset, count):
    if count >= 3:
        return offset + 1
    if count == 2:
        return jnp.abs(offset)
    return offset * 0


def own_kind(count):
    return 1 if count >= 3 else 0


def steps_of(count):
    if count >= 3:
        return ((0, -1), (2, 1))
    return ((1, 1),) if count == 2 else ()


AXES = ("gx", "gy", "gz")
MESH = pl.DeviceIdType.MESH


def neighbour(axis, count, step):
    return {axis: lax.rem(lax.axis_index(axis) + step + count, count)}


def greet(sizes):
    barrier = pltpu.get_barrier_semaphore()
    total = 0
    for axis, count in zip(AXES, sizes):
        for kind, step in steps_of(count):
            pl.semaphore_signal(barrier, inc=1, device_id=neighbour(axis, count, step), device_id_type=MESH)
            total += 1
    if total:
        pl.semaphore_wait(barrier, total)


def facing(kind, count):
    return 2 - kind if count >= 3 else kind


def spread_kernel(sizes, pos, mass, near, local_sem, send_sem, recv_sem):
    nx, ny, nz = sizes
    own = tuple(own_kind(n) for n in sizes)

    def place(i, j, k):
        return (i * kinds(ny) + j) * kinds(nz) + k

    home = place(*own)
    first = pltpu.make_async_copy(pos, near.at[home, pl.ds(0, 3)], local_sem.at[0])
    second = pltpu.make_async_copy(mass, near.at[home, pl.ds(3, 1)], local_sem.at[1])
    first.start()
    second.start()
    greet(sizes)
    first.wait()
    second.wait()
    copies = {}

    def pass_on(slot, dim):
        count = sizes[dim]
        for kind, step in steps_of(count):
            there = list(slot)
            there[dim] = facing(kind, count)
            target = place(*there)
            copy = pltpu.make_async_remote_copy(
                src_ref=near.at[place(*slot)],
                dst_ref=near.at[target],
                send_sem=send_sem.at[target],
                recv_sem=recv_sem.at[target],
                device_id=neighbour(AXES[dim], count, step),
                device_id_type=MESH,
            )
            copy.start()
            copies[tuple(there)] = copy

    order_y = [j for j in range(kinds(ny)) if j != own[1]]
    order_x = [i for i in range(kinds(nx)) if i != own[0]]
    order_z = [k for k in range(kinds(nz)) if k != own[2]]
    pass_on(own, 1)
    pass_on(own, 0)
    pass_on(own, 2)
    for j in order_y:
        slot = (own[0], j, own[2])
        copies[slot].wait_recv()
        pass_on(slot, 0)
        pass_on(slot, 2)
    for j in [own[1]] + order_y:
        for i in order_x:
            slot = (i, j, own[2])
            copies[slot].wait_recv()
            pass_on(slot, 2)
    for j in [own[1]] + order_y:
        for i in [own[0]] + order_x:
            for k in order_z:
                copies[(i, j, k)].wait_recv()
    for copy in copies.values():
        copy.wait_send()


def gather_kernel(sizes, moved, out, part, got_z, got_x, got_y, send_z, recv_z, send_x, recv_x, send_y, recv_y):
    nx, ny, nz = sizes
    own = tuple(own_kind(n) for n in sizes)

    def place(i, j, k):
        return (i * kinds(ny) + j) * kinds(nz) + k

    order_y = [j for j in range(kinds(ny)) if j != own[1]]
    order_x = [i for i in range(kinds(nx)) if i != own[0]]
    order_z = [k for k in range(kinds(nz)) if k != own[2]]
    columns = [(i, j) for j in order_y + [own[1]] for i in order_x]
    columns += [(own[0], j) for j in order_y + [own[1]]]
    greet(sizes)
    copies = []

    def send(src, dst, sends, recvs, at, dim, kind):
        count = sizes[dim]
        step = dict(steps_of(count))[kind]
        copy = pltpu.make_async_remote_copy(
            src_ref=src,
            dst_ref=dst,
            send_sem=sends.at[at],
            recv_sem=recvs.at[at],
            device_id=neighbour(AXES[dim], count, step),
            device_id_type=MESH,
        )
        copy.start()
        copies.append(copy)
        return copy

    along_z, along_x, along_y = {}, {}, {}
    for i, j in columns:
        for k in order_z:
            at = place(i, j, k)
            along_z[i, j, k] = send(moved.at[at], got_z.at[at], send_z, recv_z, at, 2, k)
    for i, j in columns:
        total = moved[place(i, j, own[2])]
        for k in order_z:
            along_z[i, j, k].wait_recv()
            total = total + got_z[place(i, j, k)]
        at = i * kinds(ny) + j
        part[at] = total
        if i != own[0]:
            along_x[i, j] = send(part.at[at], got_x.at[at], send_x, recv_x, at, 0, i)
    for j in order_y + [own[1]]:
        at = own[0] * kinds(ny) + j
        total = part[at]
        for i in order_x:
            along_x[i, j].wait_recv()
            total = total + got_x[i * kinds(ny) + j]
        part[at] = total
        if j != own[1]:
            along_y[j] = send(part.at[at], got_y.at[j], send_y, recv_y, j, 1, j)
    total = part[own[0] * kinds(ny) + own[1]]
    for j in order_y:
        along_y[j].wait_recv()
        total = total + got_y[j]
    out[...] = total
    for copy in copies:
        copy.wait_send()


def split3(value):
    first = value.astype(jnp.bfloat16).astype(jnp.float32)
    rest = value - first
    second = rest.astype(jnp.bfloat16).astype(jnp.float32)
    return first, second, rest - second


def rows_of(rows):
    at = lax.broadcasted_iota(jnp.int32, (8, 128), 0)
    out = jnp.zeros((8, 128), jnp.float32)
    for i, row in enumerate(rows):
        out = jnp.where(at == i, row, out)
    return out


def deposit_kernel(sizes, tiles_each, unroll, table, count, near, pos, radius, yields, momentum, out, acc):
    blocks, listed = pos.shape[1], table.shape[1]
    slots = near.shape[0]
    nx, ny, nz = sizes
    acc[...] = jnp.zeros_like(acc)
    live_count = count[0]
    lane = lax.broadcasted_iota(jnp.int32, (1, 128), 1)

    def one_block(b):
        row = pl.ds(b, 1)
        r = radius[row, :]
        inv = 1.0 / (r * r)
        sx, sy, sz = (pos[k, row, :] - 0.5 for k in range(3))
        left = rows_of(
            [-2.0 * inv * sx, -2.0 * inv * sy, -2.0 * inv * sz, inv, 1.0 + inv * (sx * sx + sy * sy + sz * sz)]
        )
        a1, a2, a3 = split3(left)
        lhs = jnp.concatenate([a1, a1, a2, a2, a1, a3], axis=0).T.astype(jnp.bfloat16)
        norm_acc = jnp.zeros((128, 128), jnp.float32)
        high, low, places = [], [], []
        for j in range(listed):
            tile_id = table[b, j]
            slot, tile = tile_id // tiles_each, tile_id % tiles_each
            a, bb, c = slot // 9 - 1, slot // 3 % 3 - 1, slot % 3 - 1
            place = (kind_of(a, nx) * kinds(ny) + kind_of(bb, ny)) * kinds(nz) + kind_of(c, nz)
            places.append(place * tiles_each + tile)
            at = pl.ds(tile, 1)
            gx = near[place, 0, at, :] + (a.astype(jnp.float32) - 0.5)
            gy = near[place, 1, at, :] + (bb.astype(jnp.float32) - 0.5)
            gz = near[place, 2, at, :] + (c.astype(jnp.float32) - 0.5)
            mass = near[place, 3, at, :]
            b1, b2, b3 = split3(rows_of([gx, gy, gz, gx * gx + gy * gy + gz * gz, jnp.ones_like(gx)]))
            rhs = jnp.concatenate([b1, b2, b1, b2, b3, b1], axis=0).astype(jnp.bfloat16)
            u = jnp.dot(lhs, rhs, preferred_element_type=jnp.float32)
            w = 1.0 / (u * u)
            norm_acc = norm_acc + w * mass
            w1 = w.astype(jnp.bfloat16)
            high.append(w1)
            low.append((w - w1.astype(jnp.float32)).astype(jnp.bfloat16))
        norm = jnp.sum(norm_acc.T, axis=0, keepdims=True)
        live = jnp.where(b * 128 + lane < live_count, 1.0, 0.0)
        scale = live / norm
        loads = rows_of(
            [yields[0, row, :], momentum[0, row, :], momentum[1, row, :], momentum[2, row, :], yields[1, row, :]]
        )
        c1, c2, c3 = split3(loads * scale)
        coef = jnp.concatenate([c1, c2, c3, jnp.zeros_like(c1)], axis=0).astype(jnp.bfloat16)
        for j in range(listed):
            hi = jnp.dot(coef, high[j], preferred_element_type=jnp.float32)
            lo = jnp.dot(coef[0:16], low[j], preferred_element_type=jnp.float32)
            moved = hi[0:8] + (hi[8:16] + (hi[16:24] + (lo[0:8] + lo[8:16])))
            start = pl.multiple_of(places[j] * 8, 8)
            acc[pl.ds(start, 8), :] = acc[pl.ds(start, 8), :] + moved

    def step(i, carry):
        for k in range(unroll):
            one_block(i * unroll + k)
        return carry

    used = jnp.minimum((live_count + 127) // 128, blocks)
    lax.fori_loop(0, (used + unroll - 1) // unroll, step, 0)
    for slot in range(slots):
        for q in range(5):
            out[slot, q] = acc[pl.ds(slot * tiles_each * 8 + q, tiles_each, stride=8), :]


def local(sizes, gas_pos, gas_mass, source_pos, source_radius, source_yield, source_momentum, source_tiles, source_count):
    gas_size = gas_pos.shape[-1]
    tiles = gas_size // 128
    blocks = source_pos.shape[-1] // 128
    listed = source_tiles.shape[-1]
    nx, ny, nz = sizes
    slots = kinds(nx) * kinds(ny) * kinds(nz)
    vmem = pl.BlockSpec(memory_space=pltpu.VMEM)
    near = pl.pallas_call(
        functools.partial(spread_kernel, sizes),
        out_shape=jax.ShapeDtypeStruct((slots, 4, tiles, 128), jnp.float32),
        in_specs=[vmem, vmem],
        out_specs=vmem,
        scratch_shapes=[
            pltpu.SemaphoreType.DMA((2,)),
            pltpu.SemaphoreType.DMA((slots,)),
            pltpu.SemaphoreType.DMA((slots,)),
        ],
        compiler_params=pltpu.CompilerParams(collective_id=0, has_side_effects=True),
    )(gas_pos.reshape(3, tiles, 128), gas_mass.reshape(1, tiles, 128))
    unroll = math.gcd(blocks, 4)
    smem = pl.BlockSpec(memory_space=pltpu.SMEM)
    moved = pl.pallas_call(
        functools.partial(deposit_kernel, sizes, tiles, unroll),
        out_shape=jax.ShapeDtypeStruct((slots, 5, tiles, 128), jnp.float32),
        in_specs=[smem, smem] + [vmem] * 5,
        out_specs=vmem,
        scratch_shapes=[pltpu.VMEM((slots * tiles * 8, 128), jnp.float32)],
    )(
        source_tiles.reshape(blocks, listed),
        source_count.reshape(1),
        near,
        source_pos.reshape(3, blocks, 128),
        source_radius.reshape(blocks, 128),
        source_yield.reshape(2, blocks, 128),
        source_momentum.reshape(3, blocks, 128),
    )
    piece = (5, tiles, 128)
    sides = kinds(nx) * kinds(ny)
    gain = pl.pallas_call(
        functools.partial(gather_kernel, sizes),
        out_shape=jax.ShapeDtypeStruct(piece, jnp.float32),
        in_specs=[vmem],
        out_specs=vmem,
        scratch_shapes=[
            pltpu.VMEM((sides, *piece), jnp.float32),
            pltpu.VMEM((slots, *piece), jnp.float32),
            pltpu.VMEM((sides, *piece), jnp.float32),
            pltpu.VMEM((kinds(ny), *piece), jnp.float32),
            pltpu.SemaphoreType.DMA((slots,)),
            pltpu.SemaphoreType.DMA((slots,)),
            pltpu.SemaphoreType.DMA((sides,)),
            pltpu.SemaphoreType.DMA((sides,)),
            pltpu.SemaphoreType.DMA((kinds(ny),)),
            pltpu.SemaphoreType.DMA((kinds(ny),)),
        ],
        compiler_params=pltpu.CompilerParams(collective_id=1, has_side_effects=True),
    )(moved)
    return gain.reshape(5, 1, 1, 1, gas_size)


def solution(mesh):
    sizes = (mesh.shape["gx"], mesh.shape["gy"], mesh.shape["gz"])
    in_specs = (
        P(None, "gx", "gy", "gz", None),
        P("gx", "gy", "gz", None),
        P(None, "gx", "gy", "gz", None),
        P("gx", "gy", "gz", None),
        P(None, "gx", "gy", "gz", None),
        P(None, "gx", "gy", "gz", None),
        P("gx", "gy", "gz", None, None),
        P("gx", "gy", "gz"),
    )
    out_specs = P(None, "gx", "gy", "gz", None)
    return jax.shard_map(
        functools.partial(local, sizes), mesh=mesh, in_specs=in_specs, out_specs=out_specs, check_vma=False
    )
```

```python
import functools
import math

import jax
import jax.numpy as jnp
from jax import lax
from jax.experimental import pallas as pl
from jax.experimental.pallas import tpu as pltpu
from jax.sharding import PartitionSpec as P


def kinds(count):
    return min(count, 3)


def kind_of(offset, count):
    if count >= 3:
        return offset + 1
    if count == 2:
        return jnp.abs(offset)
    return offset * 0


def own_kind(count):
    return 1 if count >= 3 else 0


def steps_of(count):
    if count >= 3:
        return ((0, -1), (2, 1))
    return ((1, 1),) if count == 2 else ()


MESH = pl.DeviceIdType.MESH


def shifted(axis, count, step):
    return lax.rem(lax.axis_index(axis) + step + count, count)


def columns_of(sizes):
    nx, ny, _ = sizes
    choices_x = steps_of(nx) + ((own_kind(nx), 0),)
    choices_y = ((own_kind(ny), 0),) + steps_of(ny)
    return [
        ((i, j), {"gx": shifted("gx", nx, dx), "gy": shifted("gy", ny, dy)})
        for i, dx in choices_x
        for j, dy in choices_y
        if dx or dy
    ]


def cores_of(sizes):
    return [(k, {"gz": shifted("gz", sizes[2], dz)}) for k, dz in steps_of(sizes[2])]


def greet(sizes):
    barrier = pltpu.get_barrier_semaphore()
    peers = columns_of(sizes) + cores_of(sizes)
    for _, device in peers:
        pl.semaphore_signal(barrier, inc=1, device_id=device, device_id_type=MESH)
    if peers:
        pl.semaphore_wait(barrier, len(peers))


def facing(kind, count):
    return 2 - kind if count >= 3 else kind


def spread_kernel(sizes, pos, mass, near, local_sem, send_sem, recv_sem):
    nx, ny, nz = sizes
    own = tuple(own_kind(n) for n in sizes)

    def place(i, j, k):
        return (i * kinds(ny) + j) * kinds(nz) + k

    home = place(*own)
    first = pltpu.make_async_copy(pos, near.at[home, pl.ds(0, 3)], local_sem.at[0])
    second = pltpu.make_async_copy(mass, near.at[home, pl.ds(3, 1)], local_sem.at[1])
    first.start()
    second.start()
    greet(sizes)
    first.wait()
    second.wait()
    copies = {}

    def send(slot, there, device):
        target = place(*there)
        copy = pltpu.make_async_remote_copy(
            src_ref=near.at[place(*slot)],
            dst_ref=near.at[target],
            send_sem=send_sem.at[target],
            recv_sem=recv_sem.at[target],
            device_id=device,
            device_id_type=MESH,
        )
        copy.start()
        copies[there] = copy

    def to_cores(i, j):
        for k, device in cores_of(sizes):
            send((i, j, own[2]), (i, j, facing(k, nz)), device)

    columns = columns_of(sizes)
    for (i, j), device in columns:
        send(own, (facing(i, nx), facing(j, ny), own[2]), device)
    to_cores(own[0], own[1])
    across = [at for at, _ in columns if at[0] != own[0]]
    along = [at for at, _ in columns if at[0] == own[0]]
    for i, j in along + across:
        copies[i, j, own[2]].wait_recv()
        to_cores(i, j)
    for i, j in [own[:2]] + along + across:
        for k, _ in steps_of(nz):
            copies[i, j, k].wait_recv()
    for copy in copies.values():
        copy.wait_send()


def gather_kernel(sizes, moved, out, part, got_z, got, send_z, recv_z, send_sem, recv_sem):
    nx, ny, nz = sizes
    own = tuple(own_kind(n) for n in sizes)

    def place(i, j, k):
        return (i * kinds(ny) + j) * kinds(nz) + k

    greet(sizes)
    copies = []

    def send(src, dst, send_at, recv_at, device):
        copy = pltpu.make_async_remote_copy(
            src_ref=src, dst_ref=dst, send_sem=send_at, recv_sem=recv_at, device_id=device, device_id_type=MESH
        )
        copy.start()
        copies.append(copy)
        return copy

    columns = columns_of(sizes)
    order = [at for at, _ in columns] + [own[:2]]
    along_z, arriving = {}, {}
    for i, j in order:
        for k, device in cores_of(sizes):
            at = place(i, j, k)
            along_z[i, j, k] = send(moved.at[at], got_z.at[at], send_z.at[at], recv_z.at[at], device)

    def send_part(index):
        (i, j), device = columns[index]
        at = i * kinds(ny) + j
        arriving[at] = send(part.at[at], got.at[at], send_sem.at[at], recv_sem.at[at], device)

    for index, (i, j) in enumerate(order):
        total = moved[place(i, j, own[2])]
        for k, _ in steps_of(nz):
            along_z[i, j, k].wait_recv()
            total = total + got_z[place(i, j, k)]
        if index < len(columns):
            part[i * kinds(ny) + j] = total
        if index:
            send_part(index - 1)
    for at in reversed(list(arriving)):
        arriving[at].wait_recv()
        total = total + got[at]
    out[...] = total
    for copy in copies:
        copy.wait_send()


def split3(value):
    first = value.astype(jnp.bfloat16).astype(jnp.float32)
    rest = value - first
    second = rest.astype(jnp.bfloat16).astype(jnp.float32)
    return first, second, rest - second


def rows_of(rows):
    at = lax.broadcasted_iota(jnp.int32, (8, 128), 0)
    out = jnp.zeros((8, 128), jnp.float32)
    for i, row in enumerate(rows):
        out = jnp.where(at == i, row, out)
    return out


def deposit_kernel(sizes, tiles_each, unroll, table, count, near, pos, radius, yields, momentum, out, acc):
    blocks, listed = pos.shape[1], table.shape[1]
    slots = near.shape[0]
    nx, ny, nz = sizes
    acc[...] = jnp.zeros_like(acc)
    live_count = count[0]
    lane = lax.broadcasted_iota(jnp.int32, (1, 128), 1)

    def one_block(b):
        row = pl.ds(b, 1)
        r = radius[row, :]
        inv = 1.0 / (r * r)
        sx, sy, sz = (pos[k, row, :] - 0.5 for k in range(3))
        left = rows_of(
            [-2.0 * inv * sx, -2.0 * inv * sy, -2.0 * inv * sz, inv, 1.0 + inv * (sx * sx + sy * sy + sz * sz)]
        )
        a1, a2, a3 = split3(left)
        lhs = jnp.concatenate([a1, a1, a2, a2, a1, a3], axis=0).T.astype(jnp.bfloat16)
        norm_acc = jnp.zeros((128, 128), jnp.float32)
        high, low, places = [], [], []
        for j in range(listed):
            tile_id = table[b, j]
            slot, tile = tile_id // tiles_each, tile_id % tiles_each
            a, bb, c = slot // 9 - 1, slot // 3 % 3 - 1, slot % 3 - 1
            place = (kind_of(a, nx) * kinds(ny) + kind_of(bb, ny)) * kinds(nz) + kind_of(c, nz)
            places.append(place * tiles_each + tile)
            at = pl.ds(tile, 1)
            gx = near[place, 0, at, :] + (a.astype(jnp.float32) - 0.5)
            gy = near[place, 1, at, :] + (bb.astype(jnp.float32) - 0.5)
            gz = near[place, 2, at, :] + (c.astype(jnp.float32) - 0.5)
            mass = near[place, 3, at, :]
            b1, b2, b3 = split3(rows_of([gx, gy, gz, gx * gx + gy * gy + gz * gz, jnp.ones_like(gx)]))
            rhs = jnp.concatenate([b1, b2, b1, b2, b3, b1], axis=0).astype(jnp.bfloat16)
            u = jnp.dot(lhs, rhs, preferred_element_type=jnp.float32)
            w = 1.0 / (u * u)
            norm_acc = norm_acc + w * mass
            w1 = w.astype(jnp.bfloat16)
            high.append(w1)
            low.append((w - w1.astype(jnp.float32)).astype(jnp.bfloat16))
        norm = jnp.sum(norm_acc.T, axis=0, keepdims=True)
        live = jnp.where(b * 128 + lane < live_count, 1.0, 0.0)
        scale = live / norm
        loads = rows_of(
            [yields[0, row, :], momentum[0, row, :], momentum[1, row, :], momentum[2, row, :], yields[1, row, :]]
        )
        c1, c2, c3 = split3(loads * scale)
        coef = jnp.concatenate([c1, c2, c3, jnp.zeros_like(c1)], axis=0).astype(jnp.bfloat16)
        for j in range(listed):
            hi = jnp.dot(coef, high[j], preferred_element_type=jnp.float32)
            lo = jnp.dot(coef[0:16], low[j], preferred_element_type=jnp.float32)
            moved = hi[0:8] + (hi[8:16] + (hi[16:24] + (lo[0:8] + lo[8:16])))
            start = pl.multiple_of(places[j] * 8, 8)
            acc[pl.ds(start, 8), :] = acc[pl.ds(start, 8), :] + moved

    def step(i, carry):
        for k in range(unroll):
            one_block(i * unroll + k)
        return carry

    used = jnp.minimum((live_count + 127) // 128, blocks)
    lax.fori_loop(0, (used + unroll - 1) // unroll, step, 0)
    for slot in range(slots):
        for q in range(5):
            out[slot, q] = acc[pl.ds(slot * tiles_each * 8 + q, tiles_each, stride=8), :]


def local(sizes, gas_pos, gas_mass, source_pos, source_radius, source_yield, source_momentum, source_tiles, source_count):
    gas_size = gas_pos.shape[-1]
    tiles = gas_size // 128
    blocks = source_pos.shape[-1] // 128
    listed = source_tiles.shape[-1]
    nx, ny, nz = sizes
    slots = kinds(nx) * kinds(ny) * kinds(nz)
    vmem = pl.BlockSpec(memory_space=pltpu.VMEM)
    near = pl.pallas_call(
        functools.partial(spread_kernel, sizes),
        out_shape=jax.ShapeDtypeStruct((slots, 4, tiles, 128), jnp.float32),
        in_specs=[vmem, vmem],
        out_specs=vmem,
        scratch_shapes=[
            pltpu.SemaphoreType.DMA((2,)),
            pltpu.SemaphoreType.DMA((slots,)),
            pltpu.SemaphoreType.DMA((slots,)),
        ],
        compiler_params=pltpu.CompilerParams(collective_id=0, has_side_effects=True),
    )(gas_pos.reshape(3, tiles, 128), gas_mass.reshape(1, tiles, 128))
    unroll = math.gcd(blocks, 4)
    smem = pl.BlockSpec(memory_space=pltpu.SMEM)
    moved = pl.pallas_call(
        functools.partial(deposit_kernel, sizes, tiles, unroll),
        out_shape=jax.ShapeDtypeStruct((slots, 5, tiles, 128), jnp.float32),
        in_specs=[smem, smem] + [vmem] * 5,
        out_specs=vmem,
        scratch_shapes=[pltpu.VMEM((slots * tiles * 8, 128), jnp.float32)],
    )(
        source_tiles.reshape(blocks, listed),
        source_count.reshape(1),
        near,
        source_pos.reshape(3, blocks, 128),
        source_radius.reshape(blocks, 128),
        source_yield.reshape(2, blocks, 128),
        source_momentum.reshape(3, blocks, 128),
    )
    piece = (5, tiles, 128)
    sides = kinds(nx) * kinds(ny)
    gain = pl.pallas_call(
        functools.partial(gather_kernel, sizes),
        out_shape=jax.ShapeDtypeStruct(piece, jnp.float32),
        in_specs=[vmem],
        out_specs=vmem,
        scratch_shapes=[
            pltpu.VMEM((sides, *piece), jnp.float32),
            pltpu.VMEM((slots, *piece), jnp.float32),
            pltpu.VMEM((sides, *piece), jnp.float32),
            pltpu.SemaphoreType.DMA((slots,)),
            pltpu.SemaphoreType.DMA((slots,)),
            pltpu.SemaphoreType.DMA((sides,)),
            pltpu.SemaphoreType.DMA((sides,)),
        ],
        compiler_params=pltpu.CompilerParams(collective_id=1, has_side_effects=True),
    )(moved)
    return gain.reshape(5, 1, 1, 1, gas_size)


def solution(mesh):
    sizes = (mesh.shape["gx"], mesh.shape["gy"], mesh.shape["gz"])
    in_specs = (
        P(None, "gx", "gy", "gz", None),
        P("gx", "gy", "gz", None),
        P(None, "gx", "gy", "gz", None),
        P("gx", "gy", "gz", None),
        P(None, "gx", "gy", "gz", None),
        P(None, "gx", "gy", "gz", None),
        P("gx", "gy", "gz", None, None),
        P("gx", "gy", "gz"),
    )
    out_specs = P(None, "gx", "gy", "gz", None)
    return jax.shard_map(
        functools.partial(local, sizes), mesh=mesh, in_specs=in_specs, out_specs=out_specs, check_vma=False
    )
```

```python
import functools
import math

import jax
import jax.numpy as jnp
from jax import lax
from jax.experimental import pallas as pl
from jax.experimental.pallas import tpu as pltpu
from jax.sharding import PartitionSpec as P


def kinds(count):
    return min(count, 3)


def kind_of(offset, count):
    if count >= 3:
        return offset + 1
    if count == 2:
        return jnp.abs(offset)
    return offset * 0


def own_kind(count):
    return 1 if count >= 3 else 0


def steps_of(count):
    if count >= 3:
        return ((0, -1), (2, 1))
    return ((1, 1),) if count == 2 else ()


MESH = pl.DeviceIdType.MESH
LIMIT = 24 * 1024 * 1024


def shifted(axis, count, step):
    return lax.rem(lax.axis_index(axis) + step + count, count)


def columns_of(sizes):
    nx, ny, _ = sizes
    choices_x = steps_of(nx) + ((own_kind(nx), 0),)
    choices_y = ((own_kind(ny), 0),) + steps_of(ny)
    return [
        ((i, j), {"gx": shifted("gx", nx, dx), "gy": shifted("gy", ny, dy)})
        for i, dx in choices_x
        for j, dy in choices_y
        if dx or dy
    ]


def cores_of(sizes):
    return [(k, {"gz": shifted("gz", sizes[2], dz)}) for k, dz in steps_of(sizes[2])]


def greet(sizes):
    barrier = pltpu.get_barrier_semaphore()
    peers = columns_of(sizes) + cores_of(sizes)
    for _, device in peers:
        pl.semaphore_signal(barrier, inc=1, device_id=device, device_id_type=MESH)
    if peers:
        pl.semaphore_wait(barrier, len(peers))


def facing(kind, count):
    return 2 - kind if count >= 3 else kind


def spread_kernel(sizes, pos, mass, near, local_sem, send_sem, recv_sem):
    nx, ny, nz = sizes
    own = tuple(own_kind(n) for n in sizes)

    def place(i, j, k):
        return (i * kinds(ny) + j) * kinds(nz) + k

    home = place(*own)
    first = pltpu.make_async_copy(pos, near.at[home, pl.ds(0, 3)], local_sem.at[0])
    second = pltpu.make_async_copy(mass, near.at[home, pl.ds(3, 1)], local_sem.at[1])
    first.start()
    second.start()
    greet(sizes)
    first.wait()
    second.wait()
    copies = {}

    def send(slot, there, device):
        target = place(*there)
        copy = pltpu.make_async_remote_copy(
            src_ref=near.at[place(*slot)],
            dst_ref=near.at[target],
            send_sem=send_sem.at[target],
            recv_sem=recv_sem.at[target],
            device_id=device,
            device_id_type=MESH,
        )
        copy.start()
        copies[there] = copy

    def to_cores(i, j):
        for k, device in cores_of(sizes):
            send((i, j, own[2]), (i, j, facing(k, nz)), device)

    columns = columns_of(sizes)
    for (i, j), device in columns:
        send(own, (facing(i, nx), facing(j, ny), own[2]), device)
    to_cores(own[0], own[1])
    across = [at for at, _ in columns if at[0] != own[0]]
    along = [at for at, _ in columns if at[0] == own[0]]
    for i, j in along + across:
        copies[i, j, own[2]].wait_recv()
        to_cores(i, j)
    for i, j in [own[:2]] + along + across:
        for k, _ in steps_of(nz):
            copies[i, j, k].wait_recv()
    for copy in copies.values():
        copy.wait_send()


def gather_kernel(sizes, moved, out, part, got_z, got, send_z, recv_z, send_sem, recv_sem):
    nx, ny, nz = sizes
    own = tuple(own_kind(n) for n in sizes)

    def place(i, j, k):
        return (i * kinds(ny) + j) * kinds(nz) + k

    greet(sizes)
    copies = []

    def send(src, dst, send_at, recv_at, device):
        copy = pltpu.make_async_remote_copy(
            src_ref=src, dst_ref=dst, send_sem=send_at, recv_sem=recv_at, device_id=device, device_id_type=MESH
        )
        copy.start()
        copies.append(copy)
        return copy

    columns = columns_of(sizes)
    order = [at for at, _ in columns] + [own[:2]]
    along_z, arriving = {}, {}
    for i, j in order:
        for k, device in cores_of(sizes):
            at = place(i, j, k)
            along_z[i, j, k] = send(moved.at[at], got_z.at[at], send_z.at[at], recv_z.at[at], device)

    def send_part(index):
        (i, j), device = columns[index]
        at = i * kinds(ny) + j
        arriving[at] = send(part.at[at], got.at[at], send_sem.at[at], recv_sem.at[at], device)

    for index, (i, j) in enumerate(order):
        total = moved[place(i, j, own[2])]
        for k, _ in steps_of(nz):
            along_z[i, j, k].wait_recv()
            total = total + got_z[place(i, j, k)]
        if index < len(columns):
            part[i * kinds(ny) + j] = total
        if index:
            send_part(index - 1)
    for at in reversed(list(arriving)):
        arriving[at].wait_recv()
        total = total + got[at]
    out[...] = total
    for copy in copies:
        copy.wait_send()


def split3(value):
    first = value.astype(jnp.bfloat16).astype(jnp.float32)
    rest = value - first
    second = rest.astype(jnp.bfloat16).astype(jnp.float32)
    return first, second, rest - second


def rows_of(rows):
    at = lax.broadcasted_iota(jnp.int32, (8, 128), 0)
    out = jnp.zeros((8, 128), jnp.float32)
    for i, row in enumerate(rows):
        out = jnp.where(at == i, row, out)
    return out


def deposit_kernel(sizes, tiles_each, unroll, table, count, near, pos, radius, yields, momentum, out, acc):
    blocks, listed = pos.shape[1], table.shape[0]
    slots = near.shape[0]
    nx, ny, nz = sizes
    acc[...] = jnp.zeros_like(acc)
    live_count = count[0]
    lane = lax.broadcasted_iota(jnp.int32, (1, 128), 1)

    def one_block(b):
        row = pl.ds(b, 1)
        r = radius[row, :]
        inv = 1.0 / (r * r)
        sx, sy, sz = (pos[k, row, :] - 0.5 for k in range(3))
        left = rows_of(
            [-2.0 * inv * sx, -2.0 * inv * sy, -2.0 * inv * sz, inv, 1.0 + inv * (sx * sx + sy * sy + sz * sz)]
        )
        a1, a2, a3 = split3(left)
        lhs = jnp.concatenate([a1, a1, a2, a2, a1, a3], axis=0).T.astype(jnp.bfloat16)
        norm_acc = jnp.zeros((128, 128), jnp.float32)
        high, low, places = [], [], []
        for j in range(listed):
            tile_id = table[j, b]
            slot, tile = tile_id // tiles_each, tile_id % tiles_each
            a, bb, c = slot // 9 - 1, slot // 3 % 3 - 1, slot % 3 - 1
            place = (kind_of(a, nx) * kinds(ny) + kind_of(bb, ny)) * kinds(nz) + kind_of(c, nz)
            places.append(place * tiles_each + tile)
            at = pl.ds(tile, 1)
            gx = near[place, 0, at, :] + (a.astype(jnp.float32) - 0.5)
            gy = near[place, 1, at, :] + (bb.astype(jnp.float32) - 0.5)
            gz = near[place, 2, at, :] + (c.astype(jnp.float32) - 0.5)
            mass = near[place, 3, at, :]
            b1, b2, b3 = split3(rows_of([gx, gy, gz, gx * gx + gy * gy + gz * gz, jnp.ones_like(gx)]))
            rhs = jnp.concatenate([b1, b2, b1, b2, b3, b1], axis=0).astype(jnp.bfloat16)
            u = jnp.dot(lhs, rhs, preferred_element_type=jnp.float32)
            w = 1.0 / (u * u)
            norm_acc = norm_acc + w * mass
            w1 = w.astype(jnp.bfloat16)
            high.append(w1)
            low.append((w - w1.astype(jnp.float32)).astype(jnp.bfloat16))
        norm = jnp.sum(norm_acc.T, axis=0, keepdims=True)
        live = jnp.where(b * 128 + lane < live_count, 1.0, 0.0)
        scale = live / norm
        loads = rows_of(
            [yields[0, row, :], momentum[0, row, :], momentum[1, row, :], momentum[2, row, :], yields[1, row, :]]
        )
        c1, c2, c3 = split3(loads * scale)
        coef = jnp.concatenate([c1, c2, c3, jnp.zeros_like(c1)], axis=0).astype(jnp.bfloat16)
        for j in range(listed):
            hi = jnp.dot(coef, high[j], preferred_element_type=jnp.float32)
            lo = jnp.dot(coef[0:16], low[j], preferred_element_type=jnp.float32)
            moved = hi[0:8] + (hi[8:16] + (hi[16:24] + (lo[0:8] + lo[8:16])))
            start = pl.multiple_of(places[j] * 8, 8)
            acc[pl.ds(start, 8), :] = acc[pl.ds(start, 8), :] + moved

    def step(i, carry):
        for k in range(unroll):
            one_block(i * unroll + k)
        return carry

    used = jnp.minimum((live_count + 127) // 128, blocks)
    lax.fori_loop(0, (used + unroll - 1) // unroll, step, 0)
    for slot in range(slots):
        for q in range(5):
            out[slot, q] = acc[pl.ds(slot * tiles_each * 8 + q, tiles_each, stride=8), :]


def local(sizes, gas_pos, gas_mass, source_pos, source_radius, source_yield, source_momentum, source_tiles, source_count):
    gas_size = gas_pos.shape[-1]
    tiles = gas_size // 128
    blocks = source_pos.shape[-1] // 128
    listed = source_tiles.shape[-1]
    nx, ny, nz = sizes
    slots = kinds(nx) * kinds(ny) * kinds(nz)
    vmem = pl.BlockSpec(memory_space=pltpu.VMEM)
    near = pl.pallas_call(
        functools.partial(spread_kernel, sizes),
        out_shape=pltpu.VMEM((slots, 4, tiles, 128), jnp.float32),
        in_specs=[vmem, vmem],
        out_specs=vmem,
        scratch_shapes=[
            pltpu.SemaphoreType.DMA((2,)),
            pltpu.SemaphoreType.DMA((slots,)),
            pltpu.SemaphoreType.DMA((slots,)),
        ],
        compiler_params=pltpu.CompilerParams(collective_id=0, has_side_effects=True, vmem_limit_bytes=LIMIT),
    )(gas_pos.reshape(3, tiles, 128), gas_mass.reshape(1, tiles, 128))
    unroll = math.gcd(blocks, 4)
    smem = pl.BlockSpec(memory_space=pltpu.SMEM)
    moved = pl.pallas_call(
        functools.partial(deposit_kernel, sizes, tiles, unroll),
        out_shape=pltpu.VMEM((slots, 5, tiles, 128), jnp.float32),
        in_specs=[smem, smem] + [vmem] * 5,
        out_specs=vmem,
        scratch_shapes=[pltpu.VMEM((slots * tiles * 8, 128), jnp.float32)],
        compiler_params=pltpu.CompilerParams(vmem_limit_bytes=LIMIT),
    )(
        source_tiles.reshape(blocks, listed).T,
        source_count.reshape(1),
        near,
        source_pos.reshape(3, blocks, 128),
        source_radius.reshape(blocks, 128),
        source_yield.reshape(2, blocks, 128),
        source_momentum.reshape(3, blocks, 128),
    )
    piece = (5, tiles, 128)
    sides = kinds(nx) * kinds(ny)
    gain = pl.pallas_call(
        functools.partial(gather_kernel, sizes),
        out_shape=jax.ShapeDtypeStruct(piece, jnp.float32),
        in_specs=[vmem],
        out_specs=vmem,
        scratch_shapes=[
            pltpu.VMEM((sides, *piece), jnp.float32),
            pltpu.VMEM((slots, *piece), jnp.float32),
            pltpu.VMEM((sides, *piece), jnp.float32),
            pltpu.SemaphoreType.DMA((slots,)),
            pltpu.SemaphoreType.DMA((slots,)),
            pltpu.SemaphoreType.DMA((sides,)),
            pltpu.SemaphoreType.DMA((sides,)),
        ],
        compiler_params=pltpu.CompilerParams(collective_id=1, has_side_effects=True, vmem_limit_bytes=LIMIT),
    )(moved)
    return gain.reshape(5, 1, 1, 1, gas_size)


def solution(mesh):
    sizes = (mesh.shape["gx"], mesh.shape["gy"], mesh.shape["gz"])
    in_specs = (
        P(None, "gx", "gy", "gz", None),
        P("gx", "gy", "gz", None),
        P(None, "gx", "gy", "gz", None),
        P("gx", "gy", "gz", None),
        P(None, "gx", "gy", "gz", None),
        P(None, "gx", "gy", "gz", None),
        P("gx", "gy", "gz", None, None),
        P("gx", "gy", "gz"),
    )
    out_specs = P(None, "gx", "gy", "gz", None)
    return jax.shard_map(
        functools.partial(local, sizes), mesh=mesh, in_specs=in_specs, out_specs=out_specs, check_vma=False
    )
```
